32 devices in a mesh: groups: 2 (over x), az: 16 (over z, y, core).
Axes of the slice: x: 2, y: 2, z: 4, core: 2. Of those that a mesh axis runs over, the one named last changes fastest.
Arguments:
- sweep_stack: bfloat16 [2, 4, 32, 80, 2560], P(None, None, ('groups', 'az')), parts along dimension 2
- blend_curve: bfloat16 [32, 80], P(('groups', 'az')), parts along dimension 0, may hold values from 0.25 to 4
- sweep_start_index: int32 [32], P(('groups', 'az')), parts along dimension 0, may hold values from -20 to 610, as said below
- usable_azimuth_extent: int32 [32, 2], P(('groups', 'az')), parts along dimension 0, may hold values from 0 to 80, as said below
- usable_column_extent: int32 [32, 2], P(('groups', 'az')), parts along dimension 0, may hold values from 0 to 2560, as said below
- image_couples: int32 [8, 2], P('groups'), parts along dimension 0, may hold values from 0 to 3, as said below
Outputs:
- interferogram: float32 [2, 8, 128, 128], P(None, 'groups', 'az'), parts along dimension 1
- coherence: float32 [8, 128, 128], P('groups', 'az'), parts along dimension 0
The draws below stay inside these ranges and needn't reach their ends.
There are 2 independent parts, one for each index of `groups`. The reference program is written for one: setup_inputs(seed, part) draws one part's arguments, and reference() takes and returns one part's arrays. A program takes and returns all parts, laid end to end along the dimension named above; each array names one. Nothing has to cross between parts.
Inputs may be any that keep to these rules, and one draw needn't show every extreme that they name: `sweep_start_index`: the valid lines of burst b lie at merged rows from b * 40 - 15 to (b + 1) * 40 + 14, and some burst reaches both ends. The valid lines of all bursts together cover every merged row from 0 to 639. `usable_azimuth_extent`: first below end for every burst. `usable_column_extent`: first below end for every burst. `image_couples`: the two acquisitions of a pair differ.
All inputs are finite; a program needn't handle non-finite values.
Results may differ from the reference program's by a relative error of at most 0.0003.
Values may be sent and summed in bfloat16 or wider, within the bound.
A program may use at most 64 MiB of HBM per device.

```python
import math
import jax
import jax.numpy as jnp
from jax import lax

BLOCK_HEIGHT = 40
SLANT_WIDTH = 2560
IMAGE_TOTAL = 4
PAIRS = 4
LOOK_ROWS = 5
LOOK_COLS = 20
SHIFT_BOUND_MAX = 10
SPILL_REACH = 5
SWEEP_HEIGHT = 80
SWEEP_TOTAL = 16
GRID_HEIGHT = 640


def geometry(key):
    seed_stream = jax.random.split(jax.random.fold_in(key, 7), 5)
    index_grid = jnp.arange(SWEEP_TOTAL + 1, dtype=jnp.int32)
    sweep_identifiers = jnp.arange(SWEEP_TOTAL, dtype=jnp.int32)
    edge_shifts = jax.random.randint(seed_stream[0], (SWEEP_TOTAL + 1,), 0 - SHIFT_BOUND_MAX, SHIFT_BOUND_MAX + 1, dtype=jnp.int32)
    peak_amount = jax.random.randint(seed_stream[1], (), 1, SWEEP_TOTAL - 1, dtype=jnp.int32)
    edge_shifts = jnp.where(index_grid == peak_amount, 0 - SHIFT_BOUND_MAX, edge_shifts)
    edge_shifts = jnp.where(index_grid == peak_amount + 1, SHIFT_BOUND_MAX, edge_shifts)
    edge_shifts = jnp.where((index_grid == 0) | (index_grid == SWEEP_TOTAL), 0, edge_shifts)
    sweep_edges = index_grid * BLOCK_HEIGHT + edge_shifts
    south_spill = jax.random.randint(seed_stream[2], (SWEEP_TOTAL,), 1, SPILL_REACH + 1, dtype=jnp.int32)
    south_spill = jnp.where(sweep_identifiers == peak_amount, SPILL_REACH, south_spill)
    north_spill = jax.random.randint(seed_stream[3], (SWEEP_TOTAL,), 1, SPILL_REACH + 1, dtype=jnp.int32)
    north_spill = jnp.where(sweep_identifiers == peak_amount, SPILL_REACH, north_spill)
    head_indices = jax.random.randint(seed_stream[4], (SWEEP_TOTAL,), 0, SPILL_REACH + 1, dtype=jnp.int32)
    start_indices = sweep_edges[:SWEEP_TOTAL] - south_spill - head_indices
    closing_indices = head_indices + south_spill + (sweep_edges[1:] - sweep_edges[:SWEEP_TOTAL]) + north_spill
    return (start_indices, head_indices, closing_indices)


def draw_sweep_start_index(key, part):
    return geometry(key)[0].astype(jnp.int32)


def draw_usable_azimuth_extent(key, part):
    start_indices, head_indices, closing_indices = geometry(key)
    return jnp.stack([head_indices, closing_indices], axis=1).astype(jnp.int32)


def draw_usable_column_extent(key, part):
    seed_stream = jax.random.split(jax.random.fold_in(key, 13), 2)
    least_index = jax.random.randint(seed_stream[0], (SWEEP_TOTAL,), 0, SLANT_WIDTH // 4, dtype=jnp.int32)
    cutoff_index = jax.random.randint(seed_stream[1], (SWEEP_TOTAL,), 0, SLANT_WIDTH // 4, dtype=jnp.int32)
    return jnp.stack([least_index, SLANT_WIDTH - cutoff_index], axis=1).astype(jnp.int32)


def draw_image_couples(key, part):
    seed_stream = jax.random.split(jax.random.fold_in(key, 17), 2)
    first_acq = jax.random.randint(seed_stream[0], (PAIRS,), 0, IMAGE_TOTAL, dtype=jnp.int32)
    step_acq = jax.random.randint(seed_stream[1], (PAIRS,), 1, IMAGE_TOTAL, dtype=jnp.int32)
    return jnp.stack([first_acq, (first_acq + step_acq) % IMAGE_TOTAL], axis=1).astype(jnp.int32)


def draw_sweep_stack(key, part):
    seed_stream = jax.random.split(jax.random.fold_in(key, 11), 4)
    result_dims = (2, IMAGE_TOTAL, SWEEP_TOTAL, SWEEP_HEIGHT, SLANT_WIDTH)
    common_indices = jax.random.normal(seed_stream[0], (2, 1, SWEEP_TOTAL, SWEEP_HEIGHT, SLANT_WIDTH), jnp.float32)
    single = jax.random.normal(seed_stream[1], result_dims, jnp.float32)
    mixture = 0.7 * (common_indices + single)
    azimuth_scale = jnp.exp(jax.random.uniform(seed_stream[2], (SWEEP_TOTAL, SWEEP_HEIGHT), jnp.float32, -0.7, 0.7))
    sample_scale = jnp.exp(jax.random.uniform(seed_stream[3], (SLANT_WIDTH,), jnp.float32, -0.7, 0.7))
    scaled = mixture * azimuth_scale[None, None, :, :, None] * sample_scale
    return scaled.astype(jnp.bfloat16)


def steps_of(stream_key, dims, pieces, smallest, top_value):
    factor_of = 1.0
    for position, parts in pieces:
        draws = jax.random.uniform(jax.random.fold_in(jax.random.fold_in(stream_key, 6), position), (parts,), jnp.float32, smallest / len(pieces), top_value / len(pieces))
        factor_of = factor_of * jnp.repeat(jnp.exp(draws), dims[position] // parts).reshape((-1,) + (1,) * (len(dims) - 1 - position))
    return factor_of


def setup_inputs(seed: int = 0, part: int = 0) -> dict:
    keys = jax.random.split(jax.random.key(seed), 7)
    part_splits = jax.random.split(jax.random.fold_in(keys[6], part), 7)
    sweep_stack = draw_sweep_stack(jax.random.fold_in(jax.random.fold_in(keys[6], part), 71), part)
    blend_curve = jnp.clip(jnp.exp(math.log(4.0) - 2.7725887 * jax.random.uniform(part_splits[1], (SWEEP_TOTAL, SWEEP_HEIGHT), jnp.float32) ** steps_of(part_splits[1], (SWEEP_TOTAL, SWEEP_HEIGHT), ((0, 16),), -0.2, 0.2)), 0.25, 4.0).astype(jnp.bfloat16)
    sweep_start_index = draw_sweep_start_index(jax.random.fold_in(jax.random.fold_in(keys[6], part), 71), part)
    usable_azimuth_extent = draw_usable_azimuth_extent(jax.random.fold_in(jax.random.fold_in(keys[6], part), 71), part)
    usable_column_extent = draw_usable_column_extent(jax.random.fold_in(jax.random.fold_in(keys[6], part), 71), part)
    image_couples = draw_image_couples(jax.random.fold_in(jax.random.fold_in(keys[6], part), 71), part)
    return dict(sweep_stack=sweep_stack, blend_curve=blend_curve, sweep_start_index=sweep_start_index, usable_azimuth_extent=usable_azimuth_extent, usable_column_extent=usable_column_extent, image_couples=image_couples)


def box_sums(values):
    shaped = values.reshape(values.shape[:-2] + (GRID_HEIGHT // LOOK_ROWS, LOOK_ROWS, SLANT_WIDTH // LOOK_COLS, LOOK_COLS))
    return jnp.sum(shaped, axis=(-3, -1))


def reference(sweep_stack, blend_curve, sweep_start_index, usable_azimuth_extent, usable_column_extent, image_couples):
    azimuth_index = jnp.arange(SWEEP_HEIGHT, dtype=jnp.int32)
    column_index = jnp.arange(SLANT_WIDTH, dtype=jnp.int32)
    reference_point = jnp.zeros((), jnp.int32)
    cross_term = jnp.zeros((2, IMAGE_TOTAL, GRID_HEIGHT + 2 * SWEEP_HEIGHT, SLANT_WIDTH), jnp.float32)
    intensity_norm = jnp.zeros((GRID_HEIGHT + 2 * SWEEP_HEIGHT,), jnp.float32)

    def deposit_sweep(sweep_index, cumulative_sums):
        aggregate, blend_total = cumulative_sums
        sweep_content = lax.dynamic_index_in_dim(sweep_stack, sweep_index, 2, keepdims=False)
        usable_marks = (azimuth_index >= usable_azimuth_extent[sweep_index, 0]) & (azimuth_index < usable_azimuth_extent[sweep_index, 1])
        azimuth_blend = jnp.where(usable_marks, blend_curve[sweep_index], jnp.zeros((), jnp.bfloat16)).astype(jnp.float32)
        column_usable = ((column_index >= usable_column_extent[sweep_index, 0]) & (column_index < usable_column_extent[sweep_index, 1])).astype(jnp.float32)
        added_term = sweep_content.astype(jnp.float32) * azimuth_blend[:, None] * column_usable[None, :]
        start_index = (sweep_start_index[sweep_index] + SWEEP_HEIGHT).astype(jnp.int32)
        available = lax.dynamic_slice(aggregate, (reference_point, reference_point, start_index, reference_point), (2, IMAGE_TOTAL, SWEEP_HEIGHT, SLANT_WIDTH))
        aggregate = lax.dynamic_update_slice(aggregate, available + added_term, (reference_point, reference_point, start_index, reference_point))
        available_blends = lax.dynamic_slice(blend_total, (start_index,), (SWEEP_HEIGHT,))
        blend_total = lax.dynamic_update_slice(blend_total, available_blends + azimuth_blend, (start_index,))
        return aggregate, blend_total

    cross_term, intensity_norm = lax.fori_loop(0, SWEEP_TOTAL, deposit_sweep, (cross_term, intensity_norm))
    combined_grid = cross_term[:, :, SWEEP_HEIGHT:SWEEP_HEIGHT + GRID_HEIGHT] / intensity_norm[SWEEP_HEIGHT:SWEEP_HEIGHT + GRID_HEIGHT][:, None]
    intensity = combined_grid[0] * combined_grid[0] + combined_grid[1] * combined_grid[1]
    first_image = jnp.take(combined_grid, image_couples[:, 0], axis=1)
    second_image = jnp.take(combined_grid, image_couples[:, 1], axis=1)
    real_part = first_image[0] * second_image[0] + first_image[1] * second_image[1]
    imag_part = first_image[1] * second_image[0] - first_image[0] * second_image[1]
    look_sum = box_sums(jnp.stack([real_part, imag_part]))
    look_power = box_sums(intensity)
    power_first = jnp.take(look_power, image_couples[:, 0], axis=0)
    power_second = jnp.take(look_power, image_couples[:, 1], axis=0)
    coherence = (look_sum[0] * look_sum[0] + look_sum[1] * look_sum[1]) / jnp.maximum(power_first * power_second, 1.0)
    interferogram = look_sum / (LOOK_ROWS * LOOK_COLS)
    return interferogram, coherence
```

```python
import functools

import jax
import jax.numpy as jnp
from jax import lax
from jax.experimental import pallas as pl
from jax.experimental.pallas import tpu as pltpu
from jax.sharding import PartitionSpec as P

BLOCK_HEIGHT = 40
LOOK_ROWS = 5
LOOK_COLS = 20
MARGIN = 15
SLOT = 16
LANES = 128
CHUNKS = 4
MESH = pl.DeviceIdType.MESH
NT = (((1,), (1,)), ((), ()))


def row_of(index, boxes):
    return (index % boxes) * LOOK_ROWS + index // boxes


def kernel(
    n, start_ref, lines_ref, samples_ref, couples_ref, curve_ref, stack_ref,
    inter_ref, coher_ref,
    lines, sent, received, own, merged, looks, column_box, power, weight_out, weight_in,
    read_sem, send_sem, recv_sem, weight_send_sem, weight_recv_sem,
):
    me = lax.axis_index("az")
    parts, images, _, height, width = lines.shape
    pairs = couples_ref.shape[1]
    rows = BLOCK_HEIGHT
    boxes = rows // LOOK_ROWS
    step = width // CHUNKS
    has_down, has_up = me > 0, me < n - 1

    def columns(chunk):
        return pl.ds(chunk * step, step)

    def read(chunk):
        return pltpu.make_async_copy(
            stack_ref.at[:, :, :, :, columns(chunk)],
            lines.at[:, :, :, :, columns(chunk)],
            read_sem.at[chunk],
        )

    for chunk in range(CHUNKS):
        read(chunk).start()

    sides = ((0, has_down, me - 1, has_up), (1, has_up, me + 1, has_down))

    barrier = pltpu.get_barrier_semaphore()
    for side, has_target, target, _ in sides:
        @pl.when(has_target)
        def _():
            pl.semaphore_signal(
                barrier, inc=1, device_id={"az": target}, device_id_type=MESH
            )

    shift = start_ref[0] - me * rows
    slot_index = lax.broadcasted_iota(jnp.int32, (LANES, height), 0)
    line_index = lax.broadcasted_iota(jnp.int32, (LANES, height), 1)
    slot_row = jnp.where(
        slot_index < SLOT,
        jnp.where(slot_index < MARGIN, slot_index - MARGIN, -1000000),
        jnp.where(slot_index < SLOT + MARGIN, slot_index - SLOT + rows, -1000000),
    )
    select = jnp.where(line_index + shift == slot_row, 1.0, 0.0)
    out_index = lax.broadcasted_iota(jnp.int32, (rows, height), 0)
    out_line = lax.broadcasted_iota(jnp.int32, (rows, height), 1)
    curve_line = lax.broadcasted_iota(jnp.int32, (8, height), 1)
    curve = jnp.where(
        (curve_line >= lines_ref[0, 0]) & (curve_line < lines_ref[0, 1]),
        jnp.broadcast_to(curve_ref[...].astype(jnp.float32), (8, height)),
        0.0,
    )
    own_weights = jnp.where(
        out_line + shift == row_of(out_index, boxes),
        jnp.broadcast_to(curve[:1], (rows, height)),
        0.0,
    )
    own_total = jnp.sum(own_weights, axis=1, keepdims=True)
    operator = jnp.concatenate([select[: 2 * SLOT], own_weights], axis=0).astype(jnp.bfloat16)
    weight_out[...] = lax.dot_general(
        curve.astype(jnp.bfloat16), select.astype(jnp.bfloat16), NT,
        preferred_element_type=jnp.float32,
    )

    pl.semaphore_wait(barrier, has_down.astype(jnp.int32) + has_up.astype(jnp.int32))

    def weight_copy(side, target):
        return pltpu.make_async_remote_copy(
            src_ref=weight_out, dst_ref=weight_in.at[side],
            send_sem=weight_send_sem.at[side], recv_sem=weight_recv_sem.at[side],
            device_id={"az": target}, device_id_type=MESH,
        )

    def line_copy(side, chunk, target):
        span = pl.ds(side * SLOT, SLOT)
        return pltpu.make_async_remote_copy(
            src_ref=sent.at[:, span, columns(chunk)],
            dst_ref=received.at[:, span, columns(chunk)],
            send_sem=send_sem.at[side, chunk], recv_sem=recv_sem.at[side, chunk],
            device_id={"az": target}, device_id_type=MESH,
        )

    for side, has_target, target, _ in sides:
        @pl.when(has_target)
        def _():
            weight_copy(side, target).start()

    for chunk in range(CHUNKS):
        read(chunk).wait()
        sample = lax.broadcasted_iota(jnp.int32, (height, step), 1) + chunk * step
        keep = jnp.where(
            (sample >= samples_ref[0, 0]) & (sample < samples_ref[0, 1]), 1.0, 0.0
        ).astype(jnp.bfloat16)
        for c in range(parts):
            for a in range(images):
                image = c * images + a
                placed = jnp.dot(
                    operator, lines[c, a, 0, :, columns(chunk)] * keep,
                    preferred_element_type=jnp.float32,
                )
                sent[image, :, columns(chunk)] = placed[: 2 * SLOT].astype(jnp.bfloat16)
                own[image, :, columns(chunk)] = placed[2 * SLOT :]
        for side, has_target, target, _ in sides:
            @pl.when(has_target)
            def _():
                line_copy(side, chunk, target).start()

    for chunk in range(CHUNKS):
        sample = lax.broadcasted_iota(jnp.int32, (step, LANES), 0) + chunk * step
        low = lax.broadcasted_iota(jnp.int32, (step, LANES), 1) * LOOK_COLS
        column_box[chunk] = jnp.where(
            (sample >= low) & (sample < low + LOOK_COLS), 1.0, 0.0
        ).astype(jnp.bfloat16)

    for side, _, _, has_source in sides:
        @pl.when(jnp.logical_not(has_source))
        def _():
            weight_in[side] = jnp.zeros_like(weight_in[side])
            span = pl.ds(side * SLOT, SLOT)
            received[:, span, :] = jnp.zeros_like(received[:, span, :])

        @pl.when(has_source)
        def _():
            weight_copy(side, me).wait_recv()

    lane = lax.broadcasted_iota(jnp.int32, (rows, LANES), 1)
    row = row_of(lax.broadcasted_iota(jnp.int32, (rows, LANES), 0), boxes)
    taken = jnp.where(
        lane < SLOT,
        jnp.broadcast_to(weight_in[0][:1], (rows, LANES)),
        jnp.broadcast_to(weight_in[1][:1], (rows, LANES)),
    )
    target_row = jnp.where(lane < SLOT, lane + rows - MARGIN, lane - SLOT)
    spill = jnp.where((target_row == row) & (lane < 2 * SLOT), taken, 0.0)
    scale = jnp.broadcast_to(
        1.0 / (own_total + jnp.sum(spill, axis=1, keepdims=True)), (rows, LANES)
    )
    spill = spill[:, : 2 * SLOT].astype(jnp.bfloat16)

    def box_rows(values):
        return jnp.sum(values.reshape(LOOK_ROWS, boxes, LANES), axis=0)

    first = [couples_ref[0, p] for p in range(pairs)]
    second = [couples_ref[1, p] for p in range(pairs)]
    total = jnp.zeros(((2 * pairs + images) * boxes, LANES), jnp.float32)
    for chunk in range(CHUNKS):
        for side, _, _, has_source in sides:
            @pl.when(has_source)
            def _():
                line_copy(side, chunk, me).wait_recv()
        for image in range(parts * images):
            arrived = jnp.dot(
                spill, received[image, :, columns(chunk)],
                preferred_element_type=jnp.float32,
            )
            for tile in range(step // LANES):
                span = pl.ds(chunk * step + tile * LANES, LANES)
                merged[image, tile] = (
                    own[image, :, span] + arrived[:, tile * LANES : (tile + 1) * LANES]
                ) * scale
        for tile in range(step // LANES):
            span = pl.ds(tile * LANES, LANES)
            for p in range(pairs):
                re1, im1 = merged[first[p], tile], merged[first[p] + images, tile]
                re2, im2 = merged[second[p], tile], merged[second[p] + images, tile]
                looks[p, :, span] = box_rows(re1 * re2 + im1 * im2)
                looks[pairs + p, :, span] = box_rows(im1 * re2 - re1 * im2)
            for a in range(images):
                re, im = merged[a, tile], merged[images + a, tile]
                looks[2 * pairs + a, :, span] = box_rows(re * re + im * im)
        values = looks[...].reshape(total.shape[0], step)
        high = values.astype(jnp.bfloat16)
        rest = (values - high.astype(jnp.float32)).astype(jnp.bfloat16)
        box = column_box[chunk]
        total += jnp.dot(high, box, preferred_element_type=jnp.float32)
        total += jnp.dot(rest, box, preferred_element_type=jnp.float32)

    total = total.reshape(2 * pairs + images, boxes, LANES)
    power[...] = total[2 * pairs :]
    for p in range(pairs):
        re, im = total[p], total[pairs + p]
        inter_ref[0, p] = re / (LOOK_ROWS * LOOK_COLS)
        inter_ref[1, p] = im / (LOOK_ROWS * LOOK_COLS)
        coher_ref[p] = (re * re + im * im) / jnp.maximum(
            power[first[p]] * power[second[p]], 1.0
        )

    for side, has_target, target, _ in sides:
        @pl.when(has_target)
        def _():
            weight_copy(side, target).wait_send()
            for chunk in range(CHUNKS):
                line_copy(side, chunk, target).wait_send()


def per_device(
    n,
    sweep_stack,
    blend_curve,
    sweep_start_index,
    usable_azimuth_extent,
    usable_column_extent,
    image_couples,
):
    parts, images, _, height, width = sweep_stack.shape
    pairs = image_couples.shape[0]
    boxes = BLOCK_HEIGHT // LOOK_ROWS
    step = width // CHUNKS
    smem = pl.BlockSpec(memory_space=pltpu.SMEM)
    vmem = pl.BlockSpec(memory_space=pltpu.VMEM)
    count = parts * images
    return pl.pallas_call(
        functools.partial(kernel, n),
        out_shape=(
            jax.ShapeDtypeStruct((2, pairs, boxes, LANES), jnp.float32),
            jax.ShapeDtypeStruct((pairs, boxes, LANES), jnp.float32),
        ),
        in_specs=[smem, smem, smem, smem, vmem, pl.BlockSpec(memory_space=pl.ANY)],
        out_specs=(vmem, vmem),
        scratch_shapes=[
            pltpu.VMEM(sweep_stack.shape, jnp.bfloat16),
            pltpu.VMEM((count, 2 * SLOT, width), jnp.bfloat16),
            pltpu.VMEM((count, 2 * SLOT, width), jnp.bfloat16),
            pltpu.VMEM((count, BLOCK_HEIGHT, width), jnp.float32),
            pltpu.VMEM((count, step // LANES, BLOCK_HEIGHT, LANES), jnp.float32),
            pltpu.VMEM((2 * pairs + images, boxes, step), jnp.float32),
            pltpu.VMEM((CHUNKS, step, LANES), jnp.bfloat16),
            pltpu.VMEM((images, boxes, LANES), jnp.float32),
            pltpu.VMEM((8, LANES), jnp.float32),
            pltpu.VMEM((2, 8, LANES), jnp.float32),
            pltpu.SemaphoreType.DMA((CHUNKS,)),
            pltpu.SemaphoreType.DMA((2, CHUNKS)),
            pltpu.SemaphoreType.DMA((2, CHUNKS)),
            pltpu.SemaphoreType.DMA((2,)),
            pltpu.SemaphoreType.DMA((2,)),
        ],
        compiler_params=pltpu.CompilerParams(collective_id=0, has_side_effects=True),
    )(
        sweep_start_index,
        usable_azimuth_extent,
        usable_column_extent,
        image_couples.T,
        blend_curve,
        sweep_stack,
    )


def solution(mesh):
    return jax.shard_map(
        functools.partial(per_device, mesh.shape["az"]),
        mesh=mesh,
        in_specs=(
            P(None, None, ("groups", "az"), None, None),
            P(("groups", "az"), None),
            P(("groups", "az")),
            P(("groups", "az"), None),
            P(("groups", "az"), None),
            P("groups", None),
        ),
        out_specs=(P(None, "groups", "az", None), P("groups", "az", None)),
        check_vma=False,
    )
```

```python
import functools

import jax
import jax.numpy as jnp
from jax import lax
from jax.experimental import pallas as pl
from jax.experimental.pallas import tpu as pltpu
from jax.sharding import PartitionSpec as P

BLOCK_HEIGHT = 40
LOOK_ROWS = 5
LOOK_COLS = 20
MARGIN = 15
SLOT = 16
LANES = 128
CHUNKS = 10
MESH = pl.DeviceIdType.MESH
NT = (((1,), (1,)), ((), ()))


def row_of(index, boxes):
    return (index % boxes) * LOOK_ROWS + index // boxes


def kernel(
    n, start_ref, lines_ref, samples_ref, couples_ref, curve_ref, stack_ref,
    inter_ref, coher_ref,
    lines, sent, received, own, merged, looks, column_box, power, weight_out, weight_in, start,
    start_sem, read_sem, send_sem, recv_sem, weight_send_sem, weight_recv_sem,
):
    me = lax.axis_index("az")
    parts, images, _, height, width = lines.shape
    pairs = couples_ref.shape[1]
    rows = BLOCK_HEIGHT
    boxes = rows // LOOK_ROWS
    step = width // CHUNKS
    has_down, has_up = me > 0, me < n - 1

    def columns(chunk):
        return pl.ds(chunk * step, step)

    def read(chunk):
        return pltpu.make_async_copy(
            stack_ref.at[:, :, :, :, columns(chunk)],
            lines.at[:, :, :, :, columns(chunk)],
            read_sem.at[chunk],
        )

    start_read = pltpu.make_async_copy(start_ref, start, start_sem.at[0])
    start_read.start()
    for chunk in range(CHUNKS):
        read(chunk).start()

    sides = ((0, has_down, me - 1, has_up), (1, has_up, me + 1, has_down))

    barrier = pltpu.get_barrier_semaphore()
    for side, has_target, target, _ in sides:
        @pl.when(has_target)
        def _():
            pl.semaphore_signal(
                barrier, inc=1, device_id={"az": target}, device_id_type=MESH
            )

    start_read.wait()
    shift = start[0] - me * rows
    slot_index = lax.broadcasted_iota(jnp.int32, (LANES, height), 0)
    line_index = lax.broadcasted_iota(jnp.int32, (LANES, height), 1)
    slot_row = jnp.where(
        slot_index < SLOT,
        jnp.where(slot_index < MARGIN, slot_index - MARGIN, -1000000),
        jnp.where(slot_index < SLOT + MARGIN, slot_index - SLOT + rows, -1000000),
    )
    select = jnp.where(line_index + shift == slot_row, 1.0, 0.0)
    out_index = lax.broadcasted_iota(jnp.int32, (rows, height), 0)
    out_line = lax.broadcasted_iota(jnp.int32, (rows, height), 1)
    curve_line = lax.broadcasted_iota(jnp.int32, (8, height), 1)
    curve = jnp.where(
        (curve_line >= lines_ref[0, 0]) & (curve_line < lines_ref[0, 1]),
        jnp.broadcast_to(curve_ref[...].astype(jnp.float32), (8, height)),
        0.0,
    )
    own_weights = jnp.where(
        out_line + shift == row_of(out_index, boxes),
        jnp.broadcast_to(curve[:1], (rows, height)),
        0.0,
    )
    own_total = jnp.sum(own_weights, axis=1, keepdims=True)
    operator = jnp.concatenate([select[: 2 * SLOT], own_weights], axis=0).astype(jnp.bfloat16)
    weight_out[...] = lax.dot_general(
        curve.astype(jnp.bfloat16), select.astype(jnp.bfloat16), NT,
        preferred_element_type=jnp.float32,
    )

    pl.semaphore_wait(barrier, has_down.astype(jnp.int32) + has_up.astype(jnp.int32))

    def weight_copy(side, target):
        return pltpu.make_async_remote_copy(
            src_ref=weight_out, dst_ref=weight_in.at[side],
            send_sem=weight_send_sem.at[side], recv_sem=weight_recv_sem.at[side],
            device_id={"az": target}, device_id_type=MESH,
        )

    def line_copy(side, chunk, target):
        span = pl.ds(side * SLOT, SLOT)
        return pltpu.make_async_remote_copy(
            src_ref=sent.at[:, span, columns(chunk)],
            dst_ref=received.at[:, span, columns(chunk)],
            send_sem=send_sem.at[side, chunk], recv_sem=recv_sem.at[side, chunk],
            device_id={"az": target}, device_id_type=MESH,
        )

    for side, has_target, target, _ in sides:
        @pl.when(has_target)
        def _():
            weight_copy(side, target).start()

    for chunk in range(CHUNKS):
        read(chunk).wait()
        sample = lax.broadcasted_iota(jnp.int32, (height, step), 1) + chunk * step
        keep = jnp.where(
            (sample >= samples_ref[0, 0]) & (sample < samples_ref[0, 1]), 1.0, 0.0
        ).astype(jnp.bfloat16)
        for c in range(parts):
            for a in range(images):
                image = c * images + a
                placed = jnp.dot(
                    operator, lines[c, a, 0, :, columns(chunk)] * keep,
                    preferred_element_type=jnp.float32,
                )
                sent[image, :, columns(chunk)] = placed[: 2 * SLOT].astype(jnp.bfloat16)
                own[image, :, columns(chunk)] = placed[2 * SLOT :]
        for side, has_target, target, _ in sides:
            @pl.when(has_target)
            def _():
                line_copy(side, chunk, target).start()

    for chunk in range(CHUNKS):
        sample = lax.broadcasted_iota(jnp.int32, (step, LANES), 0) + chunk * step
        low = lax.broadcasted_iota(jnp.int32, (step, LANES), 1) * LOOK_COLS
        column_box[chunk] = jnp.where(
            (sample >= low) & (sample < low + LOOK_COLS), 1.0, 0.0
        ).astype(jnp.bfloat16)

    for side, _, _, has_source in sides:
        @pl.when(jnp.logical_not(has_source))
        def _():
            weight_in[side] = jnp.zeros_like(weight_in[side])
            span = pl.ds(side * SLOT, SLOT)
            received[:, span, :] = jnp.zeros_like(received[:, span, :])

        @pl.when(has_source)
        def _():
            weight_copy(side, me).wait_recv()

    lane = lax.broadcasted_iota(jnp.int32, (rows, LANES), 1)
    row = row_of(lax.broadcasted_iota(jnp.int32, (rows, LANES), 0), boxes)
    taken = jnp.where(
        lane < SLOT,
        jnp.broadcast_to(weight_in[0][:1], (rows, LANES)),
        jnp.broadcast_to(weight_in[1][:1], (rows, LANES)),
    )
    target_row = jnp.where(lane < SLOT, lane + rows - MARGIN, lane - SLOT)
    spill = jnp.where((target_row == row) & (lane < 2 * SLOT), taken, 0.0)
    scale = jnp.broadcast_to(
        1.0 / (own_total + jnp.sum(spill, axis=1, keepdims=True)), (rows, LANES)
    )
    spill = spill[:, : 2 * SLOT].astype(jnp.bfloat16)

    def box_rows(values):
        return jnp.sum(values.reshape(LOOK_ROWS, boxes, LANES), axis=0)

    first = [couples_ref[0, p] for p in range(pairs)]
    second = [couples_ref[1, p] for p in range(pairs)]
    total = jnp.zeros(((2 * pairs + images) * boxes, LANES), jnp.float32)
    for chunk in range(CHUNKS):
        for side, _, _, has_source in sides:
            @pl.when(has_source)
            def _():
                line_copy(side, chunk, me).wait_recv()
        for image in range(parts * images):
            arrived = jnp.dot(
                spill, received[image, :, columns(chunk)],
                preferred_element_type=jnp.float32,
            )
            for tile in range(step // LANES):
                span = pl.ds(chunk * step + tile * LANES, LANES)
                merged[image, tile] = (
                    own[image, :, span] + arrived[:, tile * LANES : (tile + 1) * LANES]
                ) * scale
        for tile in range(step // LANES):
            span = pl.ds(tile * LANES, LANES)
            for p in range(pairs):
                re1, im1 = merged[first[p], tile], merged[first[p] + images, tile]
                re2, im2 = merged[second[p], tile], merged[second[p] + images, tile]
                looks[p, :, span] = box_rows(re1 * re2 + im1 * im2)
                looks[pairs + p, :, span] = box_rows(im1 * re2 - re1 * im2)
            for a in range(images):
                re, im = merged[a, tile], merged[images + a, tile]
                looks[2 * pairs + a, :, span] = box_rows(re * re + im * im)
        values = looks[...].reshape(total.shape[0], step)
        high = values.astype(jnp.bfloat16)
        rest = (values - high.astype(jnp.float32)).astype(jnp.bfloat16)
        box = column_box[chunk]
        total += jnp.dot(high, box, preferred_element_type=jnp.float32)
        total += jnp.dot(rest, box, preferred_element_type=jnp.float32)

    total = total.reshape(2 * pairs + images, boxes, LANES)
    power[...] = total[2 * pairs :]
    for p in range(pairs):
        re, im = total[p], total[pairs + p]
        inter_ref[0, p] = re / (LOOK_ROWS * LOOK_COLS)
        inter_ref[1, p] = im / (LOOK_ROWS * LOOK_COLS)
        coher_ref[p] = (re * re + im * im) / jnp.maximum(
            power[first[p]] * power[second[p]], 1.0
        )

    for side, has_target, target, _ in sides:
        @pl.when(has_target)
        def _():
            weight_copy(side, target).wait_send()
            for chunk in range(CHUNKS):
                line_copy(side, chunk, target).wait_send()


def per_device(
    n,
    sweep_stack,
    blend_curve,
    sweep_start_index,
    usable_azimuth_extent,
    usable_column_extent,
    image_couples,
):
    parts, images, _, height, width = sweep_stack.shape
    pairs = image_couples.shape[0]
    boxes = BLOCK_HEIGHT // LOOK_ROWS
    step = width // CHUNKS
    smem = pl.BlockSpec(memory_space=pltpu.SMEM)
    vmem = pl.BlockSpec(memory_space=pltpu.VMEM)
    hbm = pl.BlockSpec(memory_space=pltpu.HBM)
    count = parts * images
    return pl.pallas_call(
        functools.partial(kernel, n),
        out_shape=(
            pltpu.VMEM((2, pairs, boxes, LANES), jnp.float32),
            pltpu.VMEM((pairs, boxes, LANES), jnp.float32),
        ),
        in_specs=[hbm, smem, smem, smem, vmem, hbm],
        out_specs=(vmem, vmem),
        scratch_shapes=[
            pltpu.VMEM(sweep_stack.shape, jnp.bfloat16),
            pltpu.VMEM((count, 2 * SLOT, width), jnp.bfloat16),
            pltpu.VMEM((count, 2 * SLOT, width), jnp.bfloat16),
            pltpu.VMEM((count, BLOCK_HEIGHT, width), jnp.float32),
            pltpu.VMEM((count, step // LANES, BLOCK_HEIGHT, LANES), jnp.float32),
            pltpu.VMEM((2 * pairs + images, boxes, step), jnp.float32),
            pltpu.VMEM((CHUNKS, step, LANES), jnp.bfloat16),
            pltpu.VMEM((images, boxes, LANES), jnp.float32),
            pltpu.VMEM((8, LANES), jnp.float32),
            pltpu.VMEM((2, 8, LANES), jnp.float32),
            pltpu.SMEM((1,), jnp.int32),
            pltpu.SemaphoreType.DMA((1,)),
            pltpu.SemaphoreType.DMA((CHUNKS,)),
            pltpu.SemaphoreType.DMA((2, CHUNKS)),
            pltpu.SemaphoreType.DMA((2, CHUNKS)),
            pltpu.SemaphoreType.DMA((2,)),
            pltpu.SemaphoreType.DMA((2,)),
        ],
        compiler_params=pltpu.CompilerParams(
            collective_id=0, has_side_effects=True
        ),
    )(
        sweep_start_index,
        usable_azimuth_extent,
        usable_column_extent,
        image_couples.T,
        blend_curve,
        sweep_stack,
    )


def solution(mesh):
    return jax.shard_map(
        functools.partial(per_device, mesh.shape["az"]),
        mesh=mesh,
        in_specs=(
            P(None, None, ("groups", "az"), None, None),
            P(("groups", "az"), None),
            P(("groups", "az")),
            P(("groups", "az"), None),
            P(("groups", "az"), None),
            P("groups", None),
        ),
        out_specs=(P(None, "groups", "az", None), P("groups", "az", None)),
        check_vma=False,
    )
```

```python
import functools

import jax
import jax.numpy as jnp
from jax import lax
from jax.experimental import pallas as pl
from jax.experimental.pallas import tpu as pltpu
from jax.sharding import PartitionSpec as P

BLOCK_HEIGHT = 40
LOOK_ROWS = 5
LOOK_COLS = 20
MARGIN = 15
SLOT = 16
LANES = 128
CHUNKS = 10
MESH = pl.DeviceIdType.MESH
NT = (((1,), (1,)), ((), ()))


def row_of(index, boxes):
    return (index % boxes) * LOOK_ROWS + index // boxes


def kernel(
    n, start_ref, lines_ref, samples_ref, couples_ref, curve_ref, stack_ref,
    inter_ref, coher_ref,
    lines, sent, received, sent_rest, received_rest, own, merged, looks, column_box, power, weight_out, weight_in, start,
    start_sem, read_sem, send_sem, recv_sem, rest_send_sem, rest_recv_sem, weight_send_sem, weight_recv_sem,
):
    me = lax.axis_index("az")
    parts, images, _, height, width = lines.shape
    pairs = couples_ref.shape[1]
    rows = BLOCK_HEIGHT
    boxes = rows // LOOK_ROWS
    step = width // CHUNKS
    has_down, has_up = me > 0, me < n - 1

    def columns(chunk):
        return pl.ds(chunk * step, step)

    def read(chunk):
        return pltpu.make_async_copy(
            stack_ref.at[:, :, :, :, columns(chunk)],
            lines.at[:, :, :, :, columns(chunk)],
            read_sem.at[chunk],
        )

    start_read = pltpu.make_async_copy(start_ref, start, start_sem.at[0])
    start_read.start()
    for chunk in range(CHUNKS):
        read(chunk).start()

    sides = ((0, has_down, me - 1, has_up), (1, has_up, me + 1, has_down))

    barrier = pltpu.get_barrier_semaphore()
    for side, has_target, target, _ in sides:
        @pl.when(has_target)
        def _():
            pl.semaphore_signal(
                barrier, inc=1, device_id={"az": target}, device_id_type=MESH
            )

    start_read.wait()
    shift = start[0] - me * rows
    slot_index = lax.broadcasted_iota(jnp.int32, (LANES, height), 0)
    line_index = lax.broadcasted_iota(jnp.int32, (LANES, height), 1)
    slot_row = jnp.where(
        slot_index < SLOT,
        jnp.where(slot_index < MARGIN, slot_index - MARGIN, -1000000),
        jnp.where(slot_index < SLOT + MARGIN, slot_index - SLOT + rows, -1000000),
    )
    select = jnp.where(line_index + shift == slot_row, 1.0, 0.0)
    out_index = lax.broadcasted_iota(jnp.int32, (rows, height), 0)
    out_line = lax.broadcasted_iota(jnp.int32, (rows, height), 1)
    curve_line = lax.broadcasted_iota(jnp.int32, (8, height), 1)
    curve = jnp.where(
        (curve_line >= lines_ref[0, 0]) & (curve_line < lines_ref[0, 1]),
        jnp.broadcast_to(curve_ref[...].astype(jnp.float32), (8, height)),
        0.0,
    )
    own_weights = jnp.where(
        out_line + shift == row_of(out_index, boxes),
        jnp.broadcast_to(curve[:1], (rows, height)),
        0.0,
    )
    own_total = jnp.sum(own_weights, axis=1, keepdims=True)
    operator = jnp.concatenate([select[: 2 * SLOT], own_weights], axis=0).astype(jnp.bfloat16)
    half = SLOT // 2
    last = parts * images - 1
    slots = lax.broadcasted_iota(jnp.int32, (2 * SLOT, step), 0)
    turned = jnp.concatenate(
        [select[side * SLOT + MARGIN - half : side * SLOT + MARGIN] if part == 0 else
         select[side * SLOT : side * SLOT + half] for side in (0, 1) for part in (0, 1)],
        axis=0,
    )
    last_operator = jnp.concatenate([turned, own_weights], axis=0).astype(jnp.bfloat16)
    weight_out[...] = lax.dot_general(
        curve.astype(jnp.bfloat16), select.astype(jnp.bfloat16), NT,
        preferred_element_type=jnp.float32,
    )

    pl.semaphore_wait(barrier, has_down.astype(jnp.int32) + has_up.astype(jnp.int32))

    def weight_copy(side, target):
        return pltpu.make_async_remote_copy(
            src_ref=weight_out, dst_ref=weight_in.at[side],
            send_sem=weight_send_sem.at[side], recv_sem=weight_recv_sem.at[side],
            device_id={"az": target}, device_id_type=MESH,
        )

    def line_copy(side, chunk, target):
        span = pl.ds(side * SLOT, SLOT)
        return pltpu.make_async_remote_copy(
            src_ref=sent.at[:, span, columns(chunk)],
            dst_ref=received.at[:, span, columns(chunk)],
            send_sem=send_sem.at[side, chunk], recv_sem=recv_sem.at[side, chunk],
            device_id={"az": target}, device_id_type=MESH,
        )

    def rest_copy(side, chunk, target):
        span = pl.ds(side * SLOT, SLOT)
        part = pl.ds(chunk * step // 2, step // 2)
        return pltpu.make_async_remote_copy(
            src_ref=sent_rest.at[span, part], dst_ref=received_rest.at[span, part],
            send_sem=rest_send_sem.at[side, chunk], recv_sem=rest_recv_sem.at[side, chunk],
            device_id={"az": target}, device_id_type=MESH,
        )

    for side, has_target, target, _ in sides:
        @pl.when(has_target)
        def _():
            weight_copy(side, target).start()

    for chunk in range(CHUNKS):
        read(chunk).wait()
        sample = lax.broadcasted_iota(jnp.int32, (height, step), 1) + chunk * step
        keep = jnp.where(
            (sample >= samples_ref[0, 0]) & (sample < samples_ref[0, 1]), 1.0, 0.0
        ).astype(jnp.bfloat16)
        for image in range(last, -1, -1):
            placed = jnp.dot(
                last_operator if image == last else operator,
                lines[image // images, image % images, 0, :, columns(chunk)] * keep,
                preferred_element_type=jnp.float32,
            )
            own[image, :, columns(chunk)] = placed[2 * SLOT :]
            if image == last:
                extra = placed[: 2 * SLOT]
                sent_rest[:, pl.ds(chunk * step // 2, step // 2)] = jnp.concatenate(
                    [extra[side * SLOT : side * SLOT + half, part * step // 2 : (part + 1) * step // 2]
                     for side in (0, 1) for part in (0, 1)], axis=0,
                ).astype(jnp.bfloat16)
            else:
                fill = placed[: 2 * SLOT]
                for side in (0, 1):
                    at = side * SLOT + half + image
                    fill = jnp.where(
                        slots == side * SLOT + MARGIN,
                        jnp.broadcast_to(extra[at : at + 1], (2 * SLOT, step)), fill,
                    )
                sent[image, :, columns(chunk)] = fill.astype(jnp.bfloat16)
        for side, has_target, target, _ in sides:
            @pl.when(has_target)
            def _():
                line_copy(side, chunk, target).start()
                rest_copy(side, chunk, target).start()

    for chunk in range(CHUNKS):
        sample = lax.broadcasted_iota(jnp.int32, (step, LANES), 0) + chunk * step
        low = lax.broadcasted_iota(jnp.int32, (step, LANES), 1) * LOOK_COLS
        column_box[chunk] = jnp.where(
            (sample >= low) & (sample < low + LOOK_COLS), 1.0, 0.0
        ).astype(jnp.bfloat16)

    for side, _, _, has_source in sides:
        @pl.when(jnp.logical_not(has_source))
        def _():
            weight_in[side] = jnp.zeros_like(weight_in[side])
            span = pl.ds(side * SLOT, SLOT)
            received[:, span, :] = jnp.zeros_like(received[:, span, :])
            received_rest[span, :] = jnp.zeros_like(received_rest[span, :])

        @pl.when(has_source)
        def _():
            weight_copy(side, me).wait_recv()

    lane = lax.broadcasted_iota(jnp.int32, (rows, LANES), 1)
    row = row_of(lax.broadcasted_iota(jnp.int32, (rows, LANES), 0), boxes)
    taken = jnp.where(
        lane < SLOT,
        jnp.broadcast_to(weight_in[0][:1], (rows, LANES)),
        jnp.broadcast_to(weight_in[1][:1], (rows, LANES)),
    )
    target_row = jnp.where(lane < SLOT, lane + rows - MARGIN, lane - SLOT)
    spill = jnp.where((target_row == row) & (lane < 2 * SLOT), taken, 0.0)
    scale = jnp.broadcast_to(
        1.0 / (own_total + jnp.sum(spill, axis=1, keepdims=True)), (rows, LANES)
    )
    spill = spill[:, : 2 * SLOT].astype(jnp.bfloat16)

    slot_from = lax.broadcasted_iota(jnp.int32, (2 * SLOT, 2 * SLOT), 0)
    slot_to = lax.broadcasted_iota(jnp.int32, (2 * SLOT, 2 * SLOT), 1)

    def moved(match):
        order = jnp.where(match, 1.0, 0.0).astype(jnp.bfloat16)
        return jnp.dot(spill, order, preferred_element_type=jnp.float32).astype(jnp.bfloat16)

    spills = [
        jnp.concatenate(
            [spill, moved((slot_to % SLOT == MARGIN) & (slot_from == slot_to - MARGIN + image))],
            axis=0,
        )
        for image in range(last)
    ]
    rest_spills = [
        moved((slot_to % SLOT // half == part)
              & (slot_from == slot_to - part * half + MARGIN - half))
        for part in (0, 1)
    ]

    def box_rows(values):
        return jnp.sum(values.reshape(LOOK_ROWS, boxes, LANES), axis=0)

    first = [couples_ref[0, p] for p in range(pairs)]
    second = [couples_ref[1, p] for p in range(pairs)]
    total = jnp.zeros(((2 * pairs + images) * boxes, LANES), jnp.float32)
    for chunk in range(CHUNKS):
        for side, _, _, has_source in sides:
            @pl.when(has_source)
            def _():
                line_copy(side, chunk, me).wait_recv()
                rest_copy(side, chunk, me).wait_recv()
        rest = received_rest[:, pl.ds(chunk * step // 2, step // 2)]
        tail = jnp.concatenate(
            [jnp.dot(matrix, rest, preferred_element_type=jnp.float32) for matrix in rest_spills],
            axis=1,
        )
        for image in range(last + 1):
            if image < last:
                arrived = jnp.dot(
                    spills[image], received[image, :, columns(chunk)],
                    preferred_element_type=jnp.float32,
                )
                tail += arrived[rows:]
            else:
                arrived = tail
            for tile in range(step // LANES):
                span = pl.ds(chunk * step + tile * LANES, LANES)
                merged[image, tile] = (
                    own[image, :, span] + arrived[:rows, tile * LANES : (tile + 1) * LANES]
                ) * scale
        for tile in range(step // LANES):
            span = pl.ds(tile * LANES, LANES)
            for p in range(pairs):
                re1, im1 = merged[first[p], tile], merged[first[p] + images, tile]
                re2, im2 = merged[second[p], tile], merged[second[p] + images, tile]
                looks[p, :, span] = box_rows(re1 * re2 + im1 * im2)
                looks[pairs + p, :, span] = box_rows(im1 * re2 - re1 * im2)
            for a in range(images):
                re, im = merged[a, tile], merged[images + a, tile]
                looks[2 * pairs + a, :, span] = box_rows(re * re + im * im)
        values = looks[...].reshape(total.shape[0], step)
        high = values.astype(jnp.bfloat16)
        rest = (values - high.astype(jnp.float32)).astype(jnp.bfloat16)
        box = column_box[chunk]
        total += jnp.dot(high, box, preferred_element_type=jnp.float32)
        total += jnp.dot(rest, box, preferred_element_type=jnp.float32)

    total = total.reshape(2 * pairs + images, boxes, LANES)
    power[...] = total[2 * pairs :]
    for p in range(pairs):
        re, im = total[p], total[pairs + p]
        inter_ref[0, p] = re / (LOOK_ROWS * LOOK_COLS)
        inter_ref[1, p] = im / (LOOK_ROWS * LOOK_COLS)
        coher_ref[p] = (re * re + im * im) / jnp.maximum(
            power[first[p]] * power[second[p]], 1.0
        )

    for side, has_target, target, _ in sides:
        @pl.when(has_target)
        def _():
            weight_copy(side, target).wait_send()
            for chunk in range(CHUNKS):
                line_copy(side, chunk, target).wait_send()
                rest_copy(side, chunk, target).wait_send()


def per_device(
    n,
    sweep_stack,
    blend_curve,
    sweep_start_index,
    usable_azimuth_extent,
    usable_column_extent,
    image_couples,
):
    parts, images, _, height, width = sweep_stack.shape
    pairs = image_couples.shape[0]
    boxes = BLOCK_HEIGHT // LOOK_ROWS
    step = width // CHUNKS
    smem = pl.BlockSpec(memory_space=pltpu.SMEM)
    vmem = pl.BlockSpec(memory_space=pltpu.VMEM)
    hbm = pl.BlockSpec(memory_space=pltpu.HBM)
    count = parts * images
    return pl.pallas_call(
        functools.partial(kernel, n),
        out_shape=(
            pltpu.VMEM((2, pairs, boxes, LANES), jnp.float32),
            pltpu.VMEM((pairs, boxes, LANES), jnp.float32),
        ),
        in_specs=[hbm, smem, smem, smem, vmem, hbm],
        out_specs=(vmem, vmem),
        scratch_shapes=[
            pltpu.VMEM(sweep_stack.shape, jnp.bfloat16),
            pltpu.VMEM((count - 1, 2 * SLOT, width), jnp.bfloat16),
            pltpu.VMEM((count - 1, 2 * SLOT, width), jnp.bfloat16),
            pltpu.VMEM((2 * SLOT, width // 2), jnp.bfloat16),
            pltpu.VMEM((2 * SLOT, width // 2), jnp.bfloat16),
            pltpu.VMEM((count, BLOCK_HEIGHT, width), jnp.float32),
            pltpu.VMEM((count, step // LANES, BLOCK_HEIGHT, LANES), jnp.float32),
            pltpu.VMEM((2 * pairs + images, boxes, step), jnp.float32),
            pltpu.VMEM((CHUNKS, step, LANES), jnp.bfloat16),
            pltpu.VMEM((images, boxes, LANES), jnp.float32),
            pltpu.VMEM((8, LANES), jnp.float32),
            pltpu.VMEM((2, 8, LANES), jnp.float32),
            pltpu.SMEM((1,), jnp.int32),
            pltpu.SemaphoreType.DMA((1,)),
            pltpu.SemaphoreType.DMA((CHUNKS,)),
            pltpu.SemaphoreType.DMA((2, CHUNKS)),
            pltpu.SemaphoreType.DMA((2, CHUNKS)),
            pltpu.SemaphoreType.DMA((2, CHUNKS)),
            pltpu.SemaphoreType.DMA((2, CHUNKS)),
            pltpu.SemaphoreType.DMA((2,)),
            pltpu.SemaphoreType.DMA((2,)),
        ],
        compiler_params=pltpu.CompilerParams(
            collective_id=0, has_side_effects=True
        ),
    )(
        sweep_start_index,
        usable_azimuth_extent,
        usable_column_extent,
        image_couples.T,
        blend_curve,
        sweep_stack,
    )


def solution(mesh):
    return jax.shard_map(
        functools.partial(per_device, mesh.shape["az"]),
        mesh=mesh,
        in_specs=(
            P(None, None, ("groups", "az"), None, None),
            P(("groups", "az"), None),
            P(("groups", "az")),
            P(("groups", "az"), None),
            P(("groups", "az"), None),
            P("groups", None),
        ),
        out_specs=(P(None, "groups", "az", None), P("groups", "az", None)),
        check_vma=False,
    )
```
